32 devices in a mesh: dp: 8 (over z, y), mp: 4 (over x, core).
Axes of the slice: x: 2, y: 2, z: 4, core: 2. Of those that a mesh axis runs over, the one named last changes fastest.
Arguments:
- queries: bfloat16 [1024, 8192], P('dp', 'mp'), may hold values from -8 to 8
- tree_keys: bfloat16 [1024, 1024], P('dp', 'mp'), may hold values from -18 to 18
- tree_values: bfloat16 [1024, 1024], P('dp', 'mp'), may hold values from -6 to 6
- cache_keys: bfloat16 [16, 4096, 1024], P('dp', None, 'mp'), may hold values from -8 to 8
- cache_values: bfloat16 [16, 4096, 1024], P('dp', None, 'mp'), may hold values from -6 to 6
- cache_lens: int32 [16], P('dp'), may hold values from 1024 to 4096, as said below
- parents: int32 [16, 64], P('dp'), may hold values from -1 to 62, as said below
- accepted_nodes: int32 [16, 8], P('dp'), may hold values from 0 to 63, as said below
- residual: bfloat16 [1024, 8192], P('dp', 'mp'), may hold values from -1.796875 to 1.796875
- out_weight: bfloat16 [8192, 8192], P('mp', 'dp'), may hold values from -0.0625 to 0.0625
Outputs:
- tree_hidden: bfloat16 [1024, 8192], P('dp', 'mp')
- accepted_hidden: bfloat16 [128, 8192], P(None, 'mp')
The draws below stay inside these ranges and needn't reach their ends.
Inputs may be any that keep to these rules, and one draw needn't show every extreme that they name: parents[r, 0] = -1 and 0 <= parents[r, i] < i for i >= 1. accepted_nodes[r, 0] = 0, the nodes of a row increase, and parents[r, accepted_nodes[r, a + 1]] = accepted_nodes[r, a]. `cache_lens`: some request has exactly 4096 filled positions.
All inputs are finite; a program needn't handle non-finite values.
Results may differ from the reference program's by a relative error of at most 0.015.
Values may be sent and summed in bfloat16 or wider, within the bound.
A program may use at most 64 MiB of HBM per device.

```python
import math
import jax
import jax.numpy as jnp
from jax import lax

D = 8192
HEADS = 64
KV_HEADS = 8
HD = 128
NODES = 64
ACC = 8
CACHE = 4096
REQUESTS = 16
ROWS = 1024


def tree_shape(key):

    def one_tree(tree_key):
        chain_key, parent_key = jax.random.split(tree_key)
        shuffled = jax.random.permutation(chain_key, NODES - 1) + 1
        chain_nodes = jnp.sort(shuffled[:ACC - 1]).astype(jnp.int32)
        positions = jnp.arange(NODES, dtype=jnp.int32)
        parent_list = jax.random.randint(parent_key, (NODES,), 0, jnp.maximum(positions, 1)).astype(jnp.int32)
        parent_list = jnp.where(positions == 0, -1, parent_list)
        previous = jnp.concatenate([jnp.zeros((1,), jnp.int32), chain_nodes[:-1]])
        parent_list = parent_list.at[chain_nodes].set(previous)
        accepted = jnp.concatenate([jnp.zeros((1,), jnp.int32), chain_nodes])
        return (parent_list, accepted)
    request_keys = jax.random.split(jax.random.fold_in(key, 11), REQUESTS)
    return jax.vmap(one_tree)(request_keys)


def draw_parents(key, part):
    return tree_shape(key)[0].astype(jnp.int32)


def draw_accepted_nodes(key, part):
    return tree_shape(key)[1].astype(jnp.int32)


def draw_cache_lens(key, part):
    length_key, chosen_key = jax.random.split(jax.random.fold_in(key, 31))
    lengths = jax.random.randint(length_key, (REQUESTS,), CACHE // 4, CACHE + 1)
    chosen = jax.random.randint(chosen_key, (), 0, REQUESTS)
    return jnp.where(jnp.arange(REQUESTS) == chosen, CACHE, lengths).astype(jnp.int32)


def draw_cache_keys(key, part):
    shape = (REQUESTS, CACHE, KV_HEADS * HD)
    values = jax.random.normal(jax.random.fold_in(key, 1), shape, jnp.float32)
    return jnp.clip(values, -8.0, 8.0).astype(jnp.bfloat16)


def draw_queries(key, part):
    shape = (REQUESTS * NODES, HEADS * HD)
    values = 1.7 * jax.random.normal(jax.random.fold_in(key, 3), shape, jnp.float32)
    return jnp.clip(values, -8.0, 8.0).astype(jnp.bfloat16)


def block_levels(rng, extent, shards, low, top_value):
    def one(position, shards_of):
        draws = jax.random.uniform(jax.random.fold_in(jax.random.fold_in(rng, 6), position), (shards_of,), jnp.float32, low / len(shards), top_value / len(shards))
        return jnp.repeat(jnp.exp(draws), extent[position] // shards_of).reshape((-1,) + (1,) * (len(extent) - position - 1))

    loudness = one(*shards[0])
    for cut in shards[1:]:
        loudness = loudness * one(*cut)
    return loudness


def normal_values(stream_key, dims, deviation, reach, shards=(), kind=jnp.bfloat16):
    result = deviation * jax.random.normal(stream_key, dims, jnp.float32)
    if shards:
        result = result * block_levels(stream_key, dims, shards, -0.22, 0.18)
    return jnp.clip(result, -reach, reach).astype(kind)


def setup_inputs(seed: int = 0) -> dict:
    key_list = jax.random.split(jax.random.key(seed), 11)
    return {
        "queries": draw_queries(jax.random.fold_in(key_list[10], 71), 0),
        "tree_keys": normal_values(key_list[1], (ROWS, KV_HEADS * HD), 3.0, 18.0, ((0, 8), (1, 4))),
        "tree_values": normal_values(key_list[2], (ROWS, KV_HEADS * HD), 1.0, 6.0, ((0, 8), (1, 4))),
        "cache_keys": draw_cache_keys(jax.random.fold_in(key_list[10], 71), 0),
        "cache_values": normal_values(key_list[4], (REQUESTS, CACHE, KV_HEADS * HD), 1.0, 6.0, ((0, 8), (2, 4))),
        "cache_lens": draw_cache_lens(jax.random.fold_in(key_list[10], 71), 0),
        "parents": draw_parents(jax.random.fold_in(key_list[10], 71), 0),
        "accepted_nodes": draw_accepted_nodes(jax.random.fold_in(key_list[10], 71), 0),
        "residual": normal_values(key_list[8], (ROWS, D), 0.3, 1.796875, ((0, 8), (1, 4))),
        "out_weight": normal_values(key_list[9], (HEADS * HD, D), (HEADS * HD) ** -0.5, 0.0625, ((0, 4), (1, 8))),
    }


neg_large = -1e+30

def ancestry(parents):
    positions = jnp.arange(NODES, dtype=jnp.int32)
    parent_hot = (parents[:, :, None] == positions[None, None, :]).astype(jnp.float32)
    reached = parent_hot + jnp.eye(NODES, dtype=jnp.float32)[None]
    for squaring in range((NODES - 1).bit_length()):
        reached = jnp.minimum(jnp.einsum('rij,rjk->rik', reached, reached, precision=lax.Precision.HIGHEST), 1.0)
    return reached > 0.5

def reference(queries, tree_keys, tree_values, cache_keys, cache_values, cache_lens, parents, accepted_nodes, residual, out_weight):
    group_size = HEADS // KV_HEADS
    scale_factor = 1.0 / math.sqrt(HD)
    ancestor = ancestry(parents)
    query_grid = queries.reshape(REQUESTS, NODES, KV_HEADS, group_size, HD)
    tree_key_grid = tree_keys.reshape(REQUESTS, NODES, KV_HEADS, HD)
    tree_value_grid = tree_values.reshape(REQUESTS, NODES, KV_HEADS, HD)
    cache_key_grid = cache_keys.reshape(REQUESTS, CACHE, KV_HEADS, HD)
    cache_value_grid = cache_values.reshape(REQUESTS, CACHE, KV_HEADS, HD)

    def one_request(request_data):
        query_one, tkey_one, tvalue_one, ckey_one, cvalue_one, cache_length, mask_one = request_data
        query_float = query_one.astype(jnp.float32)
        cache_scores = jnp.einsum('nkgd,pkd->nkgp', query_float, ckey_one.astype(jnp.float32), precision=lax.Precision.HIGHEST) * scale_factor
        live_keys = jnp.arange(CACHE, dtype=jnp.int32) < cache_length
        cache_scores = jnp.where(live_keys[None, None, None, :], cache_scores, neg_large)
        tree_scores = jnp.einsum('nkgd,jkd->nkgj', query_float, tkey_one.astype(jnp.float32), precision=lax.Precision.HIGHEST) * scale_factor
        tree_scores = jnp.where(mask_one[:, None, None, :], tree_scores, neg_large)
        row_max = jnp.maximum(lax.optimization_barrier(jnp.max(cache_scores, axis=-1)), lax.optimization_barrier(jnp.max(tree_scores, axis=-1)))
        cache_weights = jnp.exp(cache_scores - row_max[..., None])
        tree_weights = jnp.exp(tree_scores - row_max[..., None])
        denominator = lax.optimization_barrier(jnp.sum(cache_weights, axis=-1)) + lax.optimization_barrier(jnp.sum(tree_weights, axis=-1))
        rounded_cache = lax.optimization_barrier(cache_weights.astype(jnp.bfloat16)).astype(jnp.float32)
        rounded_tree = lax.optimization_barrier(tree_weights.astype(jnp.bfloat16)).astype(jnp.float32)
        numerator = jnp.einsum('nkgp,pkd->nkgd', rounded_cache, cvalue_one.astype(jnp.float32), precision=lax.Precision.HIGHEST)
        numerator = numerator + jnp.einsum('nkgj,jkd->nkgd', rounded_tree, tvalue_one.astype(jnp.float32), precision=lax.Precision.HIGHEST)
        return (numerator / denominator[..., None]).astype(jnp.bfloat16).reshape(NODES, HEADS * HD)
    attended = lax.map(one_request, (query_grid, tree_key_grid, tree_value_grid, cache_key_grid, cache_value_grid, cache_lens, ancestor))
    attended = attended.reshape(REQUESTS * NODES, HEADS * HD)
    projected = jnp.dot(attended, out_weight, preferred_element_type=jnp.float32)
    tree_hidden = (residual.astype(jnp.float32) + projected).astype(jnp.bfloat16)
    picked_rows = (jnp.arange(REQUESTS, dtype=jnp.int32)[:, None] * NODES + accepted_nodes).reshape(-1)
    accepted_hidden = jnp.take(tree_hidden, picked_rows, axis=0)
    return (tree_hidden, accepted_hidden)
```

```python
import functools
import math

import jax
import jax.numpy as jnp
from jax import lax
from jax.experimental import pallas as pl
from jax.experimental.pallas import tpu as pltpu
from jax.sharding import PartitionSpec as P

HEADS = 64
KV_HEADS = 8
HD = 128
neg_large = -1e30
MESH = pl.DeviceIdType.MESH


def attention_kernel(lens_ref, q_ref, tk_ref, tv_ref, ck_ref, cv_ref, par_ref, o_ref):
    nodes = tk_ref.shape[0]
    cache = ck_ref.shape[1]
    group = q_ref.shape[1] // HD
    block = min(1024, cache)
    factor = math.log2(math.e) / math.sqrt(HD)
    f32 = jnp.float32
    bf = jnp.bfloat16
    length = lens_ref[pl.program_id(0)]

    lane = lax.broadcasted_iota(jnp.int32, (nodes, nodes), 1)
    row = lax.broadcasted_iota(jnp.int32, (nodes, nodes), 0)
    reached = jnp.where((par_ref[0] == lane) | (row == lane), 1.0, 0.0).astype(f32)
    for _ in range((nodes - 1).bit_length()):
        hot = reached.astype(bf)
        reached = jnp.minimum(jnp.dot(hot, hot, preferred_element_type=f32), 1.0)

    parts = 2
    per = group // parts
    rows = per * nodes
    nt = (((1,), (1,)), ((), ()))

    def queries(p):
        return jnp.concatenate(
            [q_ref[:, (p * per + g) * HD : (p * per + g + 1) * HD] for g in range(per)], axis=0
        )

    def with_ones(v):
        return jnp.concatenate([v, jnp.ones(v.shape, bf)], axis=1)

    mask = jnp.concatenate([reached] * per, axis=0) > 0.5
    state = []
    for p in range(parts):
        s = lax.dot_general(queries(p), tk_ref[...], nt, preferred_element_type=f32)
        s = jnp.where(mask, s, neg_large)
        m = jnp.max(s, axis=1, keepdims=True)
        w = jnp.exp2((s - m) * factor).astype(bf)
        acc = jnp.dot(w, with_ones(tv_ref[...]), preferred_element_type=f32)
        state += [m, acc]

    def step(b, state, masked):
        start = pl.multiple_of(b * block, block)
        k = ck_ref[0, pl.ds(start, block), :]
        v = with_ones(cv_ref[0, pl.ds(start, block), :])
        out = []
        scores = [
            lax.dot_general(queries(p), k, nt, preferred_element_type=f32) for p in range(parts)
        ]
        for p in range(parts):
            m, acc = state[2 * p], state[2 * p + 1]
            s = scores[p]
            if masked:
                at = start + lax.broadcasted_iota(jnp.int32, (1, block), 1)
                s = jnp.where(at < length, s, neg_large)
            new = jnp.maximum(m, jnp.max(s, axis=1, keepdims=True))
            w = jnp.exp2((s - new) * factor).astype(bf)
            acc = acc * jnp.exp2((m - new) * factor) + jnp.dot(w, v, preferred_element_type=f32)
            out += [new, acc]
        return tuple(out)

    full = length // block
    state = lax.fori_loop(0, full, lambda b, c: step(b, c, False), tuple(state))
    state = lax.fori_loop(full, pl.cdiv(length, block), lambda b, c: step(b, c, True), state)
    for p in range(parts):
        acc = state[2 * p + 1]
        done = (acc[:, :HD] / acc[:, HD:]).astype(bf)
        for g in range(per):
            o_ref[:, (p * per + g) * HD : (p * per + g + 1) * HD] = done[
                g * nodes : (g + 1) * nodes
            ]


def attend(queries, tree_keys, tree_values, cache_keys, cache_values, cache_lens, parents):
    requests, nodes = parents.shape
    cache = cache_keys.shape[1]
    kv = tree_keys.shape[1] // HD
    wide = queries.shape[1] // kv
    return pl.pallas_call(
        attention_kernel,
        out_shape=jax.ShapeDtypeStruct(queries.shape, jnp.bfloat16),
        grid_spec=pltpu.PrefetchScalarGridSpec(
            num_scalar_prefetch=1,
            grid=(requests, kv),
            in_specs=[
                pl.BlockSpec((nodes, wide), lambda r, k, _: (r, k)),
                pl.BlockSpec((nodes, HD), lambda r, k, _: (r, k)),
                pl.BlockSpec((nodes, HD), lambda r, k, _: (r, k)),
                pl.BlockSpec((1, cache, HD), lambda r, k, _: (r, 0, k)),
                pl.BlockSpec((1, cache, HD), lambda r, k, _: (r, 0, k)),
                pl.BlockSpec((1, nodes, 1), lambda r, k, _: (r, 0, 0)),
            ],
            out_specs=pl.BlockSpec((nodes, wide), lambda r, k, _: (r, k)),
        ),
        compiler_params=pltpu.CompilerParams(vmem_limit_bytes=40 * 1024 * 1024),
        name="attention",
    )(cache_lens, queries, tree_keys, tree_values, cache_keys, cache_values, parents[:, :, None])


def per_device(
    queries,
    tree_keys,
    tree_values,
    cache_keys,
    cache_values,
    cache_lens,
    parents,
    accepted_nodes,
    residual,
    out_weight,
):
    request_count, node_count = parents.shape
    attended = attend(
        queries, tree_keys, tree_values, cache_keys, cache_values, cache_lens, parents
    )
    feature_share = residual.shape[1]
    all_rows = jnp.dot(
        lax.all_gather(attended, "dp", axis=0, tiled=True),
        out_weight,
        preferred_element_type=jnp.float32,
    )
    partial_sum = lax.all_to_all(
        all_rows.astype(jnp.bfloat16), "dp", split_axis=0, concat_axis=1, tiled=True
    ).astype(all_rows.dtype)
    head_total_sum = lax.psum(partial_sum.astype(jnp.bfloat16), "mp").astype(jnp.float32)
    own_share = lax.dynamic_slice_in_dim(
        head_total_sum, lax.axis_index("mp") * feature_share, feature_share, 1
    )
    tree_hidden = (residual.astype(jnp.float32) + own_share).astype(jnp.bfloat16)
    row_base = jnp.arange(request_count, dtype=jnp.int32)[:, None] * node_count
    picked_rows = (row_base + accepted_nodes).reshape(-1)
    picked_hidden = jnp.take(tree_hidden, picked_rows, axis=0)
    accepted_hidden = lax.all_gather(picked_hidden, "dp", axis=0, tiled=True)
    return (tree_hidden, accepted_hidden)


def solution(mesh):
    placed = (
        P("dp", "mp"),
        P("dp", "mp"),
        P("dp", "mp"),
        P("dp", None, "mp"),
        P("dp", None, "mp"),
        P("dp"),
        P("dp", None),
        P("dp", None),
        P("dp", "mp"),
        P("mp", "dp"),
    )
    return jax.shard_map(
        per_device,
        mesh=mesh,
        in_specs=placed,
        out_specs=(P("dp", "mp"), P(None, "mp")),
        check_vma=False,
    )
```

```python
import functools
import math

import jax
import jax.numpy as jnp
from jax import lax
from jax.experimental import pallas as pl
from jax.experimental.pallas import tpu as pltpu
from jax.sharding import PartitionSpec as P

HEADS = 64
KV_HEADS = 8
HD = 128
neg_large = -1e30
MESH = pl.DeviceIdType.MESH


def attention_kernel(lens_ref, q_ref, tk_ref, tv_ref, ck_ref, cv_ref, par_ref, o_ref):
    nodes = tk_ref.shape[0]
    cache = ck_ref.shape[1]
    group = q_ref.shape[1] // HD
    block = min(1024, cache)
    factor = math.log2(math.e) / math.sqrt(HD)
    f32 = jnp.float32
    bf = jnp.bfloat16
    length = lens_ref[pl.program_id(0)]

    lane = lax.broadcasted_iota(jnp.int32, (nodes, nodes), 1)
    row = lax.broadcasted_iota(jnp.int32, (nodes, nodes), 0)
    reached = jnp.where((par_ref[0] == lane) | (row == lane), 1.0, 0.0).astype(f32)
    for _ in range((nodes - 1).bit_length()):
        hot = reached.astype(bf)
        reached = jnp.minimum(jnp.dot(hot, hot, preferred_element_type=f32), 1.0)

    parts = 2
    per = group // parts
    rows = per * nodes
    nt = (((1,), (1,)), ((), ()))

    def queries(p):
        return jnp.concatenate(
            [q_ref[:, (p * per + g) * HD : (p * per + g + 1) * HD] for g in range(per)], axis=0
        )

    def with_ones(v):
        return jnp.concatenate([v, jnp.ones(v.shape, bf)], axis=1)

    mask = jnp.concatenate([reached] * per, axis=0) > 0.5
    state = []
    for p in range(parts):
        s = lax.dot_general(queries(p), tk_ref[...], nt, preferred_element_type=f32)
        s = jnp.where(mask, s, neg_large)
        m = jnp.max(s, axis=1, keepdims=True)
        w = jnp.exp2((s - m) * factor).astype(bf)
        acc = jnp.dot(w, with_ones(tv_ref[...]), preferred_element_type=f32)
        state += [m, acc]

    def step(b, state, masked):
        start = pl.multiple_of(b * block, block)
        k = ck_ref[0, pl.ds(start, block), :]
        v = with_ones(cv_ref[0, pl.ds(start, block), :])
        out = []
        scores = [
            lax.dot_general(queries(p), k, nt, preferred_element_type=f32) for p in range(parts)
        ]
        for p in range(parts):
            m, acc = state[2 * p], state[2 * p + 1]
            s = scores[p]
            if masked:
                at = start + lax.broadcasted_iota(jnp.int32, (1, block), 1)
                s = jnp.where(at < length, s, neg_large)
            new = jnp.maximum(m, jnp.max(s, axis=1, keepdims=True))
            w = jnp.exp2((s - new) * factor).astype(bf)
            acc = acc * jnp.exp2((m - new) * factor) + jnp.dot(w, v, preferred_element_type=f32)
            out += [new, acc]
        return tuple(out)

    full = length // block
    state = lax.fori_loop(0, full, lambda b, c: step(b, c, False), tuple(state))
    state = lax.fori_loop(full, pl.cdiv(length, block), lambda b, c: step(b, c, True), state)
    for p in range(parts):
        acc = state[2 * p + 1]
        done = (acc[:, :HD] / acc[:, HD:]).astype(bf)
        for g in range(per):
            o_ref[:, (p * per + g) * HD : (p * per + g + 1) * HD] = done[
                g * nodes : (g + 1) * nodes
            ]


def attend(queries, tree_keys, tree_values, cache_keys, cache_values, cache_lens, parents):
    requests, nodes = parents.shape
    cache = cache_keys.shape[1]
    kv = tree_keys.shape[1] // HD
    wide = queries.shape[1] // kv
    return pl.pallas_call(
        attention_kernel,
        out_shape=jax.ShapeDtypeStruct(queries.shape, jnp.bfloat16),
        grid_spec=pltpu.PrefetchScalarGridSpec(
            num_scalar_prefetch=1,
            grid=(requests, kv),
            in_specs=[
                pl.BlockSpec((nodes, wide), lambda r, k, _: (r, k)),
                pl.BlockSpec((nodes, HD), lambda r, k, _: (r, k)),
                pl.BlockSpec((nodes, HD), lambda r, k, _: (r, k)),
                pl.BlockSpec((1, cache, HD), lambda r, k, _: (r, 0, k)),
                pl.BlockSpec((1, cache, HD), lambda r, k, _: (r, 0, k)),
                pl.BlockSpec((1, nodes, 1), lambda r, k, _: (r, 0, 0)),
            ],
            out_specs=pl.BlockSpec((nodes, wide), lambda r, k, _: (r, k)),
        ),
        compiler_params=pltpu.CompilerParams(vmem_limit_bytes=40 * 1024 * 1024),
        name="attention",
    )(cache_lens, queries, tree_keys, tree_values, cache_keys, cache_values, parents[:, :, None])


def line_order(place, length, event):
    short = jnp.minimum(place, length - 1 - place)
    ring = (event + 1) // 2
    near = jnp.where(event % 2 == 1, place - ring, place + ring)
    far = jnp.where(place < length - 1 - place, event, length - 1 - event)
    return jnp.where(event <= 2 * short, near, far)


def project_kernel(
    dp_size,
    mp_size,
    att_ref,
    w_ref,
    res_ref,
    pick_ref,
    hid_ref,
    acc_ref,
    gathered,
    total,
    *rest,
):
    f32, bf = jnp.float32, jnp.bfloat16
    stages = (mp_size - 1).bit_length()
    outgoing, incoming = rest[:stages], rest[stages : 2 * stages]
    (
        settled, owned, picks,
        ga_send, ga_recv, st_send, st_recv, own_send, own_recv, pk_send, pk_recv,
    ) = rest[2 * stages :]
    rows = att_ref.shape[0]
    wide = w_ref.shape[1]
    share = dp_size // mp_size
    length = dp_size // 2
    d = lax.axis_index("dp")
    m = lax.axis_index("mp")
    place, side = d // 2, d % 2
    peer_side = 1 - side

    barrier = pltpu.get_barrier_semaphore()

    def greet(i, carry):
        @pl.when(i != d * mp_size + m)
        def _():
            pl.semaphore_signal(
                barrier, inc=1, device_id=(i // mp_size, i % mp_size), device_id_type=MESH
            )

        return carry

    lax.fori_loop(0, dp_size * mp_size, greet, 0)
    pl.semaphore_wait(barrier, dp_size * mp_size - 1)

    def gather_copy(src, j, way, target):
        return pltpu.make_async_remote_copy(
            src_ref=src,
            dst_ref=gathered.at[j],
            send_sem=ga_send.at[j, way],
            recv_sem=ga_recv.at[j],
            device_id=(target, m),
            device_id_type=MESH,
        )

    def spread(src, j, at, started):
        up = place + 1
        down = place - 1
        for way, ok, target in (
            (0, (at <= place) & (up < length), up * 2 + side),
            (1, (at >= place) & (down >= 0), down * 2 + side),
        ):

            @pl.when(ok)
            def _():
                copy = gather_copy(src, j, way, target)
                copy.start() if started else copy.wait_send()

        copy = gather_copy(src, j, 2, place * 2 + peer_side)
        copy.start() if started else copy.wait_send()

    def stage_copy(t, j):
        bit = 1 << t
        partner = m + bit * (1 - 2 * ((m // bit) % 2))
        return pltpu.make_async_remote_copy(
            src_ref=outgoing[t].at[j],
            dst_ref=incoming[t].at[j],
            send_sem=st_send.at[t, j],
            recv_sem=st_recv.at[t, j],
            device_id=(d, partner),
            device_id_type=MESH,
        )

    def kept(t):
        offset = 0
        for u in range(t):
            offset = offset + ((m // (1 << u)) % 2) * (rows >> (u + 1))
        return offset

    def half(t, keep):
        bit = (m // (1 << t)) % 2
        pick = bit if keep else 1 - bit
        size = rows >> (t + 1)
        return pl.ds(pl.multiple_of(kept(t) + pick * size, 16), size)

    def push(t, j):
        outgoing[t][j] = total[j, half(t, False), :].astype(bf)
        stage_copy(t, j).start()

    final = rows >> stages
    tile = min(512, wide)

    def multiply(src, j):
        @pl.loop(0, wide // tile)
        def _(n):
            cols = pl.ds(pl.multiple_of(n * tile, tile), tile)
            total[j, :, cols] = jnp.dot(src[...], w_ref[:, cols], preferred_element_type=f32)

        push(0, j)

    def final_copy(j):
        return pltpu.make_async_remote_copy(
            src_ref=settled.at[j],
            dst_ref=owned.at[d % share, m],
            send_sem=own_send.at[j],
            recv_sem=own_recv.at[d % share, m],
            device_id=(j, d // share),
            device_id_type=MESH,
        )

    def final_local(j):
        return pltpu.make_async_copy(
            settled.at[j], owned.at[d % share, m], own_recv.at[d % share, m]
        )

    def fold(t, j):
        stage_copy(t, j).wait_recv()
        keep = half(t, True)
        if t + 1 < stages:
            total[j, keep, :] = total[j, keep, :] + incoming[t][j].astype(f32)
            push(t + 1, j)
        else:
            settled[j] = (total[j, keep, :] + incoming[t][j].astype(f32)).astype(bf)
            own = (j == d) & (d // share == m)

            @pl.when(own)
            def _():
                final_local(j).start()

            @pl.when(jnp.logical_not(own))
            def _():
                final_copy(j).start()

    def own_block(e):
        return line_order(place, length, e) * 2 + side

    def peer_block(e):
        return line_order(place, length, e) * 2 + peer_side

    def block_at(k):
        if k == 0:
            return own_block(0)
        if k == dp_size - 1:
            return peer_block(length - 1)
        return own_block((k + 1) // 2) if k % 2 == 1 else peer_block(k // 2 - 1)

    spread(att_ref, d, place, True)
    for k in range(dp_size + stages):
        if k < dp_size:
            j = block_at(k)
            if k == 0:
                multiply(att_ref, j)
            else:
                gather_copy(gathered.at[j], j, 2, d * 0 + place * 2 + peer_side).wait_recv()
                if k % 2 == 1 and k < dp_size - 1:
                    spread(gathered.at[j], j, j // 2, True)
                multiply(gathered.at[j], j)
        for t in range(stages):
            b = k - 1 - t
            if 0 <= b < dp_size:
                fold(t, block_at(b))

    for i in range(share):
        cols = slice(i * wide, (i + 1) * wide)
        for p in range(mp_size):
            pltpu.make_async_copy(settled.at[0], owned.at[i, p], own_recv.at[i, p]).wait()
            start = 0
            for t in range(stages):
                start += ((p >> t) & 1) * (rows >> (t + 1))
            at = slice(start, start + final)
            hid_ref[at, cols] = (res_ref[at, cols].astype(f32) + owned[i, p].astype(f32)).astype(bf)

    count = pick_ref.shape[0]
    hot = pick_ref[...] == lax.broadcasted_iota(jnp.int32, (count, rows), 1)
    picked = jnp.dot(
        jnp.where(hot, 1.0, 0.0).astype(bf), hid_ref[...], preferred_element_type=f32
    ).astype(bf)
    picks[d] = picked

    def pick_copy(step):
        target = lax.rem(d + step, dp_size)
        return pltpu.make_async_remote_copy(
            src_ref=picks.at[d],
            dst_ref=picks.at[d],
            send_sem=pk_send.at[step],
            recv_sem=pk_recv.at[d],
            device_id=(target, m),
            device_id_type=MESH,
        )

    def pick_wait(step):
        source = lax.rem(d + step, dp_size)
        pltpu.make_async_copy(picks.at[source], picks.at[source], pk_recv.at[source]).wait()

    for step in range(1, dp_size):
        pick_copy(step).start()
    spread(att_ref, d, place, False)
    for e in range(1, length):
        j = own_block(e)
        spread(gathered.at[j], j, j // 2, False)
    for j in range(dp_size):
        for t in range(stages):
            stage_copy(t, j).wait_send()

        @pl.when(jnp.logical_not((j == d) & (d // share == m)))
        def _():
            final_copy(j).wait_send()

    acc_ref[pl.ds(pl.multiple_of(d * count, count), count), :] = picked
    for step in range(1, dp_size):
        pick_wait(step)
        source = lax.rem(d + step, dp_size)
        acc_ref[pl.ds(pl.multiple_of(source * count, count), count), :] = picks[source]
    for step in range(1, dp_size):
        pick_copy(step).wait_send()


def project(attended, out_weight, residual, picks, dp_size, mp_size):
    bf = jnp.bfloat16
    rows, depth = attended.shape
    wide = out_weight.shape[1]
    features = residual.shape[1]
    count = picks.shape[0]
    stages = (mp_size - 1).bit_length()
    share = dp_size // mp_size
    halves = [pltpu.VMEM((dp_size, rows >> (t + 1), wide), bf) for t in range(stages)]
    dma = pltpu.SemaphoreType.DMA
    vmem = pl.BlockSpec(memory_space=pltpu.VMEM)
    return pl.pallas_call(
        functools.partial(project_kernel, dp_size, mp_size),
        out_shape=(
            jax.ShapeDtypeStruct((rows, features), bf),
            jax.ShapeDtypeStruct((dp_size * count, features), bf),
        ),
        in_specs=[vmem] * 4,
        out_specs=(vmem, vmem),
        scratch_shapes=[
            pltpu.VMEM((dp_size, rows, depth), bf),
            pltpu.VMEM((dp_size, rows, wide), jnp.float32),
            *halves,
            *halves,
            pltpu.VMEM((dp_size, rows >> stages, wide), bf),
            pltpu.VMEM((share, mp_size, rows >> stages, wide), bf),
            pltpu.VMEM((dp_size, count, features), bf),
            dma((dp_size, 3)),
            dma((dp_size,)),
            dma((stages, dp_size)),
            dma((stages, dp_size)),
            dma((dp_size,)),
            dma((share, mp_size)),
            dma((dp_size,)),
            dma((dp_size,)),
        ],
        compiler_params=pltpu.CompilerParams(
            collective_id=0, has_side_effects=True, vmem_limit_bytes=56 * 1024 * 1024
        ),
        name="project",
    )(attended, out_weight, residual, picks)


def per_device(
    dp_size,
    mp_size,
    queries,
    tree_keys,
    tree_values,
    cache_keys,
    cache_values,
    cache_lens,
    parents,
    accepted_nodes,
    residual,
    out_weight,
):
    request_count, node_count = parents.shape
    attended = attend(
        queries, tree_keys, tree_values, cache_keys, cache_values, cache_lens, parents
    )
    row_base = jnp.arange(request_count, dtype=jnp.int32)[:, None] * node_count
    picks = (row_base + accepted_nodes).reshape(-1, 1)
    return project(attended, out_weight, residual, picks, dp_size, mp_size)


def solution(mesh):
    placed = (
        P("dp", "mp"),
        P("dp", "mp"),
        P("dp", "mp"),
        P("dp", None, "mp"),
        P("dp", None, "mp"),
        P("dp"),
        P("dp", None),
        P("dp", None),
        P("dp", "mp"),
        P("mp", "dp"),
    )
    return jax.shard_map(
        functools.partial(per_device, mesh.shape["dp"], mesh.shape["mp"]),
        mesh=mesh,
        in_specs=placed,
        out_specs=(P("dp", "mp"), P(None, "mp")),
        check_vma=False,
    )
```

```python
import functools
import math

import jax
import jax.numpy as jnp
from jax import lax
from jax.experimental import pallas as pl
from jax.experimental.pallas import tpu as pltpu
from jax.sharding import PartitionSpec as P

HEADS = 64
KV_HEADS = 8
HD = 128
neg_large = -1e30
VMEM_ALL = 67043328
MESH = pl.DeviceIdType.MESH


def attention_kernel(lens_ref, q_ref, tk_ref, tv_ref, ck_ref, cv_ref, par_ref, o_ref):
    nodes = tk_ref.shape[0]
    cache = ck_ref.shape[1]
    group = q_ref.shape[1] // HD
    block = min(1024, cache)
    factor = math.log2(math.e) / math.sqrt(HD)
    f32 = jnp.float32
    bf = jnp.bfloat16
    length = lens_ref[pl.program_id(0)]

    lane = lax.broadcasted_iota(jnp.int32, (nodes, nodes), 1)
    row = lax.broadcasted_iota(jnp.int32, (nodes, nodes), 0)
    reached = jnp.where((par_ref[0] == lane) | (row == lane), 1.0, 0.0).astype(f32)
    for _ in range((nodes - 1).bit_length()):
        hot = reached.astype(bf)
        reached = jnp.minimum(jnp.dot(hot, hot, preferred_element_type=f32), 1.0)

    parts = 2
    per = group // parts
    rows = per * nodes
    nt = (((1,), (1,)), ((), ()))

    def queries(p):
        return jnp.concatenate(
            [q_ref[:, (p * per + g) * HD : (p * per + g + 1) * HD] for g in range(per)], axis=0
        )

    def with_ones(v):
        return jnp.concatenate([v, jnp.ones(v.shape, bf)], axis=1)

    mask = jnp.concatenate([reached] * per, axis=0) > 0.5
    state = []
    for p in range(parts):
        s = lax.dot_general(queries(p), tk_ref[...], nt, preferred_element_type=f32)
        s = jnp.where(mask, s, neg_large)
        m = jnp.max(s, axis=1, keepdims=True)
        w = jnp.exp2((s - m) * factor).astype(bf)
        acc = jnp.dot(w, with_ones(tv_ref[...]), preferred_element_type=f32)
        state += [m, acc]

    def step(b, state, masked):
        start = pl.multiple_of(b * block, block)
        k = ck_ref[0, pl.ds(start, block), :]
        v = with_ones(cv_ref[0, pl.ds(start, block), :])
        out = []
        scores = [
            lax.dot_general(queries(p), k, nt, preferred_element_type=f32) for p in range(parts)
        ]
        for p in range(parts):
            m, acc = state[2 * p], state[2 * p + 1]
            s = scores[p]
            if masked:
                at = start + lax.broadcasted_iota(jnp.int32, (1, block), 1)
                s = jnp.where(at < length, s, neg_large)
            new = jnp.maximum(m, jnp.max(s, axis=1, keepdims=True))
            w = jnp.exp2((s - new) * factor).astype(bf)
            acc = acc * jnp.exp2((m - new) * factor) + jnp.dot(w, v, preferred_element_type=f32)
            out += [new, acc]
        return tuple(out)

    full = length // block
    state = lax.fori_loop(0, full, lambda b, c: step(b, c, False), tuple(state))
    state = lax.fori_loop(full, pl.cdiv(length, block), lambda b, c: step(b, c, True), state)
    for p in range(parts):
        acc = state[2 * p + 1]
        done = (acc[:, :HD] / acc[:, HD:]).astype(bf)
        for g in range(per):
            o_ref[:, (p * per + g) * HD : (p * per + g + 1) * HD] = done[
                g * nodes : (g + 1) * nodes
            ]


def attend(queries, tree_keys, tree_values, cache_keys, cache_values, cache_lens, parents):
    requests, nodes = parents.shape
    cache = cache_keys.shape[1]
    kv = tree_keys.shape[1] // HD
    wide = queries.shape[1] // kv
    return pl.pallas_call(
        attention_kernel,
        out_shape=jax.ShapeDtypeStruct(queries.shape, jnp.bfloat16),
        grid_spec=pltpu.PrefetchScalarGridSpec(
            num_scalar_prefetch=1,
            grid=(requests, kv),
            in_specs=[
                pl.BlockSpec((nodes, wide), lambda r, k, _: (r, k)),
                pl.BlockSpec((nodes, HD), lambda r, k, _: (r, k)),
                pl.BlockSpec((nodes, HD), lambda r, k, _: (r, k)),
                pl.BlockSpec((1, cache, HD), lambda r, k, _: (r, 0, k)),
                pl.BlockSpec((1, cache, HD), lambda r, k, _: (r, 0, k)),
                pl.BlockSpec((1, nodes, 1), lambda r, k, _: (r, 0, 0)),
            ],
            out_specs=pl.BlockSpec((nodes, wide), lambda r, k, _: (r, k)),
        ),
        compiler_params=pltpu.CompilerParams(vmem_limit_bytes=VMEM_ALL),
        name="attention",
    )(cache_lens, queries, tree_keys, tree_values, cache_keys, cache_values, parents[:, :, None])


def line_order(place, length, event):
    short = jnp.minimum(place, length - 1 - place)
    ring = (event + 1) // 2
    near = jnp.where(event % 2 == 1, place - ring, place + ring)
    far = jnp.where(place < length - 1 - place, event, length - 1 - event)
    return jnp.where(event <= 2 * short, near, far)


def project_kernel(
    dp_size,
    mp_size,
    att_ref,
    w_hbm,
    res_ref,
    pick_ref,
    hid_ref,
    acc_ref,
    gathered,
    total,
    *rest,
):
    f32, bf = jnp.float32, jnp.bfloat16
    stages = (mp_size - 1).bit_length()
    outgoing, incoming = rest[:stages], rest[stages : 2 * stages]
    (
        w_ref, w_sem, settled, owned, picks,
        ga_send, ga_recv, st_send, st_recv, own_send, own_recv, pk_send, pk_recv,
    ) = rest[2 * stages :]
    rows = att_ref.shape[0]
    wide = w_hbm.shape[1]
    share = dp_size // mp_size
    length = dp_size // 2
    d = lax.axis_index("dp")
    m = lax.axis_index("mp")
    place, side = d // 2, d % 2
    peer_side = 1 - side

    w_copy = pltpu.make_async_copy(w_hbm, w_ref, w_sem)
    w_copy.start()
    barrier = pltpu.get_barrier_semaphore()

    def greet(i, carry):
        @pl.when(i != d * mp_size + m)
        def _():
            pl.semaphore_signal(
                barrier, inc=1, device_id=(i // mp_size, i % mp_size), device_id_type=MESH
            )

        return carry

    lax.fori_loop(0, dp_size * mp_size, greet, 0)
    pl.semaphore_wait(barrier, dp_size * mp_size - 1)

    def gather_copy(src, j, way, target):
        return pltpu.make_async_remote_copy(
            src_ref=src,
            dst_ref=gathered.at[j],
            send_sem=ga_send.at[j, way],
            recv_sem=ga_recv.at[j],
            device_id=(target, m),
            device_id_type=MESH,
        )

    def spread(src, j, at, started):
        up = place + 1
        down = place - 1
        for way, ok, target in (
            (0, (at <= place) & (up < length), up * 2 + side),
            (1, (at >= place) & (down >= 0), down * 2 + side),
        ):

            @pl.when(ok)
            def _():
                copy = gather_copy(src, j, way, target)
                copy.start() if started else copy.wait_send()

        copy = gather_copy(src, j, 2, place * 2 + peer_side)
        copy.start() if started else copy.wait_send()

    def stage_copy(t, j):
        bit = 1 << t
        partner = m + bit * (1 - 2 * ((m // bit) % 2))
        return pltpu.make_async_remote_copy(
            src_ref=outgoing[t].at[j],
            dst_ref=incoming[t].at[j],
            send_sem=st_send.at[t, j],
            recv_sem=st_recv.at[t, j],
            device_id=(d, partner),
            device_id_type=MESH,
        )

    def kept(t):
        offset = 0
        for u in range(t):
            offset = offset + ((m // (1 << u)) % 2) * (rows >> (u + 1))
        return offset

    def half(t, keep):
        bit = (m // (1 << t)) % 2
        pick = bit if keep else 1 - bit
        size = rows >> (t + 1)
        return pl.ds(pl.multiple_of(kept(t) + pick * size, 16), size)

    def push(t, j):
        outgoing[t][j] = total[j, half(t, False), :].astype(bf)
        stage_copy(t, j).start()

    final = rows >> stages
    tile = min(512, wide)

    def multiply(src, j):
        @pl.loop(0, wide // tile)
        def _(n):
            cols = pl.ds(pl.multiple_of(n * tile, tile), tile)
            total[j, :, cols] = jnp.dot(src[...], w_ref[:, cols], preferred_element_type=f32)

        push(0, j)

    def final_copy(j):
        return pltpu.make_async_remote_copy(
            src_ref=settled.at[j],
            dst_ref=owned.at[d % share, m],
            send_sem=own_send.at[j],
            recv_sem=own_recv.at[d % share, m],
            device_id=(j, d // share),
            device_id_type=MESH,
        )

    def final_local(j):
        return pltpu.make_async_copy(
            settled.at[j], owned.at[d % share, m], own_recv.at[d % share, m]
        )

    def fold(t, j):
        stage_copy(t, j).wait_recv()
        keep = half(t, True)
        if t + 1 < stages:
            total[j, keep, :] = total[j, keep, :] + incoming[t][j].astype(f32)
            push(t + 1, j)
        else:
            settled[j] = (total[j, keep, :] + incoming[t][j].astype(f32)).astype(bf)
            own = (j == d) & (d // share == m)

            @pl.when(own)
            def _():
                final_local(j).start()

            @pl.when(jnp.logical_not(own))
            def _():
                final_copy(j).start()

    def own_block(e):
        return line_order(place, length, e) * 2 + side

    def peer_block(e):
        return line_order(place, length, e) * 2 + peer_side

    def block_at(k):
        if k == 0:
            return own_block(0)
        if k == dp_size - 1:
            return peer_block(length - 1)
        return own_block((k + 1) // 2) if k % 2 == 1 else peer_block(k // 2 - 1)

    spread(att_ref, d, place, True)
    w_copy.wait()
    for k in range(dp_size + stages):
        if k < dp_size:
            j = block_at(k)
            if k == 0:
                multiply(att_ref, j)
            else:
                gather_copy(gathered.at[j], j, 2, d * 0 + place * 2 + peer_side).wait_recv()
                if k % 2 == 1 and k < dp_size - 1:
                    spread(gathered.at[j], j, j // 2, True)
                multiply(gathered.at[j], j)
        for t in range(stages):
            b = k - 1 - t
            if 0 <= b < dp_size:
                fold(t, block_at(b))

    for i in range(share):
        cols = slice(i * wide, (i + 1) * wide)
        for p in range(mp_size):
            pltpu.make_async_copy(settled.at[0], owned.at[i, p], own_recv.at[i, p]).wait()
            start = 0
            for t in range(stages):
                start += ((p >> t) & 1) * (rows >> (t + 1))
            at = slice(start, start + final)
            hid_ref[at, cols] = (res_ref[at, cols].astype(f32) + owned[i, p].astype(f32)).astype(bf)

    count = pick_ref.shape[0]
    hot = pick_ref[...] == lax.broadcasted_iota(jnp.int32, (count, rows), 1)
    picked = jnp.dot(
        jnp.where(hot, 1.0, 0.0).astype(bf), hid_ref[...], preferred_element_type=f32
    ).astype(bf)
    picks[d] = picked

    def pick_copy(j, way, target):
        return pltpu.make_async_remote_copy(
            src_ref=picks.at[j],
            dst_ref=picks.at[j],
            send_sem=pk_send.at[way],
            recv_sem=pk_recv.at[j],
            device_id=(target, m),
            device_id_type=MESH,
        )

    peer = place * 2 + peer_side
    pick_copy(d, 0, peer).start()
    for e in range(1, length):
        pick_copy(d, e, own_block(e)).start()
    for e in range(1, length):
        j = own_block(e)
        pick_copy(j, length + e, peer).wait_recv()
        pick_copy(j, length + e, peer).start()
    spread(att_ref, d, place, False)
    for e in range(1, length):
        j = own_block(e)
        spread(gathered.at[j], j, j // 2, False)
    for j in range(dp_size):
        for t in range(stages):
            stage_copy(t, j).wait_send()

        @pl.when(jnp.logical_not((j == d) & (d // share == m)))
        def _():
            final_copy(j).wait_send()

    for e in range(length):
        j = peer_block(e)
        pick_copy(j, e, peer).wait_recv()
    for j in range(dp_size):
        acc_ref[j * count : (j + 1) * count, :] = picks[j]
    for e in range(length):
        pick_copy(d, e, peer).wait_send()
        if e:
            pick_copy(d, length + e, peer).wait_send()


def project(attended, out_weight, residual, picks, dp_size, mp_size):
    bf = jnp.bfloat16
    rows, depth = attended.shape
    wide = out_weight.shape[1]
    features = residual.shape[1]
    count = picks.shape[0]
    stages = (mp_size - 1).bit_length()
    share = dp_size // mp_size
    halves = [pltpu.VMEM((dp_size, rows >> (t + 1), wide), bf) for t in range(stages)]
    dma = pltpu.SemaphoreType.DMA
    vmem = pl.BlockSpec(memory_space=pltpu.VMEM)
    return pl.pallas_call(
        functools.partial(project_kernel, dp_size, mp_size),
        out_shape=(
            jax.ShapeDtypeStruct((rows, features), bf),
            jax.ShapeDtypeStruct((dp_size * count, features), bf),
        ),
        in_specs=[vmem, pl.BlockSpec(memory_space=pl.ANY), vmem, vmem],
        out_specs=(vmem, vmem),
        scratch_shapes=[
            pltpu.VMEM((dp_size, rows, depth), bf),
            pltpu.VMEM((dp_size, rows, wide), jnp.float32),
            *halves,
            *halves,
            pltpu.VMEM((depth, wide), bf),
            dma(()),
            pltpu.VMEM((dp_size, rows >> stages, wide), bf),
            pltpu.VMEM((share, mp_size, rows >> stages, wide), bf),
            pltpu.VMEM((dp_size, count, features), bf),
            dma((dp_size, 3)),
            dma((dp_size,)),
            dma((stages, dp_size)),
            dma((stages, dp_size)),
            dma((dp_size,)),
            dma((share, mp_size)),
            dma((dp_size,)),
            dma((dp_size,)),
        ],
        compiler_params=pltpu.CompilerParams(
            collective_id=0, has_side_effects=True, vmem_limit_bytes=VMEM_ALL
        ),
        name="project",
    )(attended, out_weight, residual, picks)


def per_device(
    dp_size,
    mp_size,
    queries,
    tree_keys,
    tree_values,
    cache_keys,
    cache_values,
    cache_lens,
    parents,
    accepted_nodes,
    residual,
    out_weight,
):
    request_count, node_count = parents.shape
    attended = attend(
        queries, tree_keys, tree_values, cache_keys, cache_values, cache_lens, parents
    )
    row_base = jnp.arange(request_count, dtype=jnp.int32)[:, None] * node_count
    picks = (row_base + accepted_nodes).reshape(-1, 1)
    return project(attended, out_weight, residual, picks, dp_size, mp_size)


def solution(mesh):
    placed = (
        P("dp", "mp"),
        P("dp", "mp"),
        P("dp", "mp"),
        P("dp", None, "mp"),
        P("dp", None, "mp"),
        P("dp"),
        P("dp", None),
        P("dp", None),
        P("dp", "mp"),
        P("mp", "dp"),
    )
    return jax.shard_map(
        functools.partial(per_device, mesh.shape["dp"], mesh.shape["mp"]),
        mesh=mesh,
        in_specs=placed,
        out_specs=(P("dp", "mp"), P(None, "mp")),
        check_vma=False,
    )
```

```python
import functools
import math

import jax
import jax.numpy as jnp
from jax import lax
from jax.experimental import pallas as pl
from jax.experimental.pallas import tpu as pltpu
from jax.sharding import PartitionSpec as P

HEADS = 64
KV_HEADS = 8
HD = 128
neg_large = -1e30
VMEM_ALL = 67043328
MESH = pl.DeviceIdType.MESH


def ancestry(par_ref, r):
    f32, bf = jnp.float32, jnp.bfloat16
    nodes = par_ref.shape[1]
    lane = lax.broadcasted_iota(jnp.int32, (nodes, nodes), 1)
    row = lax.broadcasted_iota(jnp.int32, (nodes, nodes), 0)
    reached = jnp.where((par_ref[r] == lane) | (row == lane), 1.0, 0.0).astype(f32)
    for _ in range((nodes - 1).bit_length()):
        hot = reached.astype(bf)
        reached = jnp.minimum(jnp.dot(hot, hot, preferred_element_type=f32), 1.0)
    return reached


def attend_unit(r, k, reached, length, q_ref, tk_ref, tv_ref, k_ref, v_ref, o_ref):
    f32, bf = jnp.float32, jnp.bfloat16
    nodes = reached.shape[0]
    cache = k_ref.shape[0]
    group = HEADS // KV_HEADS
    block = min(1024, cache)
    factor = math.log2(math.e) / math.sqrt(HD)
    parts = 2
    per = group // parts
    nt = (((1,), (1,)), ((), ()))
    line = slice(r * nodes, (r + 1) * nodes)

    def column(p, g):
        head = k * group + p * per + g
        return slice(head * HD, (head + 1) * HD)

    def queries(p):
        return jnp.concatenate([q_ref[line, column(p, g)] for g in range(per)], axis=0)

    def with_ones(v):
        return jnp.concatenate([v, jnp.ones(v.shape, bf)], axis=1)

    mask = jnp.concatenate([reached] * per, axis=0) > 0.5
    own = slice(k * HD, (k + 1) * HD)
    state = []
    for p in range(parts):
        s = lax.dot_general(queries(p), tk_ref[line, own], nt, preferred_element_type=f32)
        s = jnp.where(mask, s, neg_large)
        m = jnp.max(s, axis=1, keepdims=True)
        w = jnp.exp2((s - m) * factor).astype(bf)
        acc = jnp.dot(w, with_ones(tv_ref[line, own]), preferred_element_type=f32)
        state += [m, acc]

    def step(b, state, masked):
        start = pl.multiple_of(b * block, block)
        keys = k_ref[pl.ds(start, block), :]
        values = with_ones(v_ref[pl.ds(start, block), :])
        scores = [
            lax.dot_general(queries(p), keys, nt, preferred_element_type=f32)
            for p in range(parts)
        ]
        out = []
        for p in range(parts):
            m, acc = state[2 * p], state[2 * p + 1]
            s = scores[p]
            if masked:
                at = start + lax.broadcasted_iota(jnp.int32, (1, block), 1)
                s = jnp.where(at < length, s, neg_large)
            new = jnp.maximum(m, jnp.max(s, axis=1, keepdims=True))
            w = jnp.exp2((s - new) * factor).astype(bf)
            acc = acc * jnp.exp2((m - new) * factor) + jnp.dot(
                w, values, preferred_element_type=f32
            )
            out += [new, acc]
        return tuple(out)

    state = lax.fori_loop(0, cache // block, lambda b, c: step(b, c, True), tuple(state))
    for p in range(parts):
        acc = state[2 * p + 1]
        done = (acc[:, :HD] / acc[:, HD:]).astype(bf)
        for g in range(per):
            o_ref[line, column(p, g)] = done[g * nodes : (g + 1) * nodes]


def line_order(place, length, event):
    short = jnp.minimum(place, length - 1 - place)
    ring = (event + 1) // 2
    near = jnp.where(event % 2 == 1, place - ring, place + ring)
    far = jnp.where(place < length - 1 - place, event, length - 1 - event)
    return jnp.where(event <= 2 * short, near, far)


def project_kernel(
    dp_size,
    mp_size,
    lens_ref,
    q_ref,
    tk_ref,
    tv_ref,
    ck_ref,
    cv_ref,
    par_ref,
    w_hbm,
    res_ref,
    pick_ref,
    hid_ref,
    acc_ref,
    gathered,
    total,
    *rest,
):
    f32, bf = jnp.float32, jnp.bfloat16
    stages = (mp_size - 1).bit_length()
    outgoing, incoming = rest[:stages], rest[stages : 2 * stages]
    (
        att_ref, k_buf, v_buf, kv_sem, w_ref, w_sem, settled, owned, picks,
        ga_send, ga_recv, st_send, st_recv, own_send, own_recv, pk_send, pk_recv,
    ) = rest[2 * stages :]
    rows, depth = q_ref.shape
    requests, nodes, _ = par_ref.shape
    units = k_buf.shape[0]
    span = depth * requests // units
    wide = w_hbm.shape[1]
    share = dp_size // mp_size
    length = dp_size // 2
    d = lax.axis_index("dp")
    m = lax.axis_index("mp")
    place, side = d // 2, d % 2
    peer_side = 1 - side

    w_copy = pltpu.make_async_copy(w_hbm, w_ref, w_sem)
    loads = []
    for c in range(units):
        cols = slice(c // requests * HD, (c // requests + 1) * HD)
        pair = (
            pltpu.make_async_copy(ck_ref.at[c % requests, :, cols], k_buf.at[c], kv_sem.at[c, 0]),
            pltpu.make_async_copy(cv_ref.at[c % requests, :, cols], v_buf.at[c], kv_sem.at[c, 1]),
        )
        for load in pair:
            load.start()
        loads.append(pair)
    w_copy.start()
    barrier = pltpu.get_barrier_semaphore()

    def greet(i, carry):
        @pl.when(i != d * mp_size + m)
        def _():
            pl.semaphore_signal(
                barrier, inc=1, device_id=(i // mp_size, i % mp_size), device_id_type=MESH
            )

        return carry

    lax.fori_loop(0, dp_size * mp_size, greet, 0)
    pl.semaphore_wait(barrier, dp_size * mp_size - 1)

    def chunk(ref, c):
        r, k = c % requests, c // requests
        return ref.at[r * nodes : (r + 1) * nodes, k * span : (k + 1) * span]

    def gather_copy(src, j, c, way, target):
        return pltpu.make_async_remote_copy(
            src_ref=chunk(src, c),
            dst_ref=chunk(gathered.at[j], c),
            send_sem=ga_send.at[j, c, way],
            recv_sem=ga_recv.at[j, c],
            device_id=(target, m),
            device_id_type=MESH,
        )

    peer = place * 2 + peer_side

    def spread(src, j, c, ways, started):
        for way in ways:
            target = (place + 1 - 2 * way) * 2 + side
            ok = place < length - 1 if way == 0 else place > 0

            @pl.when(ok)
            def _():
                copy = gather_copy(src, j, c, way, target)
                copy.start() if started else copy.wait_send()

        copy = gather_copy(src, j, c, 2, peer)
        copy.start() if started else copy.wait_send()

    def relay(c, ring, started):
        for way in range(2):
            at = place - ring if way == 0 else place + ring
            j = at * 2 + side

            @pl.when(at >= 0 if way == 0 else at < length)
            def _():
                if started:
                    gather_copy(gathered.at[j], j, c, 2, peer).wait_recv()
                spread(gathered.at[j], j, c, (way,), started)

    def slot(t):
        for c in range(max(0, t - length + 1), min(t, units)):
            relay(c, t - c, True)

    def stage_copy(t, j):
        bit = 1 << t
        partner = m + bit * (1 - 2 * ((m // bit) % 2))
        return pltpu.make_async_remote_copy(
            src_ref=outgoing[t].at[j],
            dst_ref=incoming[t].at[j],
            send_sem=st_send.at[t, j],
            recv_sem=st_recv.at[t, j],
            device_id=(d, partner),
            device_id_type=MESH,
        )

    def kept(t):
        offset = 0
        for u in range(t):
            offset = offset + ((m // (1 << u)) % 2) * (rows >> (u + 1))
        return offset

    def half(t, keep):
        bit = (m // (1 << t)) % 2
        pick = bit if keep else 1 - bit
        size = rows >> (t + 1)
        return pl.ds(pl.multiple_of(kept(t) + pick * size, 16), size)

    def push(t, j):
        outgoing[t][j] = total[j, half(t, False), :].astype(bf)
        stage_copy(t, j).start()

    final = rows >> stages
    tile = min(512, wide)

    def multiply(src, j):
        @pl.loop(0, wide // tile)
        def _(n):
            cols = pl.ds(pl.multiple_of(n * tile, tile), tile)
            total[j, :, cols] = jnp.dot(src[...], w_ref[:, cols], preferred_element_type=f32)

        push(0, j)

    def final_copy(j):
        return pltpu.make_async_remote_copy(
            src_ref=settled.at[j],
            dst_ref=owned.at[d % share, m],
            send_sem=own_send.at[j],
            recv_sem=own_recv.at[d % share, m],
            device_id=(j, d // share),
            device_id_type=MESH,
        )

    def final_local(j):
        return pltpu.make_async_copy(
            settled.at[j], owned.at[d % share, m], own_recv.at[d % share, m]
        )

    def fold(t, j):
        stage_copy(t, j).wait_recv()
        keep = half(t, True)
        if t + 1 < stages:
            total[j, keep, :] = total[j, keep, :] + incoming[t][j].astype(f32)
            push(t + 1, j)
        else:
            settled[j] = (total[j, keep, :] + incoming[t][j].astype(f32)).astype(bf)
            own = (j == d) & (d // share == m)

            @pl.when(own)
            def _():
                final_local(j).start()

            @pl.when(jnp.logical_not(own))
            def _():
                final_copy(j).start()

    def own_block(e):
        return line_order(place, length, e) * 2 + side

    def peer_block(e):
        return line_order(place, length, e) * 2 + peer_side

    def block_at(k):
        if k == 0:
            return own_block(0)
        if k == dp_size - 1:
            return peer_block(length - 1)
        return own_block((k + 1) // 2) if k % 2 == 1 else peer_block(k // 2 - 1)

    trees = [ancestry(par_ref, r) for r in range(requests)]
    for c in range(units):
        r, k = c % requests, c // requests
        for load in loads[c]:
            load.wait()
        attend_unit(
            r, k, trees[r], lens_ref[r], q_ref, tk_ref, tv_ref, k_buf.at[c], v_buf.at[c], att_ref
        )
        spread(att_ref, d, c, (0, 1), True)
        slot(c)
    w_copy.wait()
    for k in range(dp_size + stages):
        if k < dp_size:
            j = block_at(k)
            if k == 0:
                multiply(att_ref, j)
            elif k % 2 == 1 and k < dp_size - 1:
                slot(units - 1 + (k + 1) // 2)
                multiply(gathered.at[j], j)
            else:
                for c in range(units):
                    gather_copy(gathered.at[j], j, c, 2, peer).wait_recv()
                multiply(gathered.at[j], j)
        for t in range(stages):
            b = k - 1 - t
            if 0 <= b < dp_size:
                fold(t, block_at(b))

    for i in range(share):
        cols = slice(i * wide, (i + 1) * wide)
        for p in range(mp_size):
            pltpu.make_async_copy(settled.at[0], owned.at[i, p], own_recv.at[i, p]).wait()
            start = 0
            for t in range(stages):
                start += ((p >> t) & 1) * (rows >> (t + 1))
            at = slice(start, start + final)
            hid_ref[at, cols] = (res_ref[at, cols].astype(f32) + owned[i, p].astype(f32)).astype(bf)

    count = pick_ref.shape[0]
    hot = pick_ref[...] == lax.broadcasted_iota(jnp.int32, (count, rows), 1)
    picked = jnp.dot(
        jnp.where(hot, 1.0, 0.0).astype(bf), hid_ref[...], preferred_element_type=f32
    ).astype(bf)
    picks[d] = picked

    def pick_copy(j, way, target):
        return pltpu.make_async_remote_copy(
            src_ref=picks.at[j],
            dst_ref=picks.at[j],
            send_sem=pk_send.at[way],
            recv_sem=pk_recv.at[j],
            device_id=(target, m),
            device_id_type=MESH,
        )

    pick_copy(d, 0, peer).start()
    for e in range(1, length):
        pick_copy(d, e, own_block(e)).start()
    for e in range(1, length):
        j = own_block(e)
        pick_copy(j, length + e, peer).wait_recv()
        pick_copy(j, length + e, peer).start()
    for c in range(units):
        spread(att_ref, d, c, (0, 1), False)
        for ring in range(1, length):
            relay(c, ring, False)
    for j in range(dp_size):
        for t in range(stages):
            stage_copy(t, j).wait_send()

        @pl.when(jnp.logical_not((j == d) & (d // share == m)))
        def _():
            final_copy(j).wait_send()

    for e in range(length):
        j = peer_block(e)
        pick_copy(j, e, peer).wait_recv()
    for j in range(dp_size):
        acc_ref[j * count : (j + 1) * count, :] = picks[j]
    for e in range(length):
        pick_copy(d, e, peer).wait_send()
        if e:
            pick_copy(d, length + e, peer).wait_send()


def project(
    lens, queries, keys, values, cache_k, cache_v, parents, out_weight, residual, picks,
    dp_size, mp_size,
):
    bf = jnp.bfloat16
    rows, depth = queries.shape
    requests, cache, _ = cache_k.shape
    units = requests * keys.shape[1] // HD
    wide = out_weight.shape[1]
    features = residual.shape[1]
    count = picks.shape[0]
    stages = (mp_size - 1).bit_length()
    share = dp_size // mp_size
    halves = [pltpu.VMEM((dp_size, rows >> (t + 1), wide), bf) for t in range(stages)]
    dma = pltpu.SemaphoreType.DMA
    vmem = pl.BlockSpec(memory_space=pltpu.VMEM)
    hbm = pl.BlockSpec(memory_space=pl.ANY)
    return pl.pallas_call(
        functools.partial(project_kernel, dp_size, mp_size),
        out_shape=(
            jax.ShapeDtypeStruct((rows, features), bf),
            jax.ShapeDtypeStruct((dp_size * count, features), bf),
        ),
        in_specs=[pl.BlockSpec(memory_space=pltpu.SMEM), vmem, vmem, vmem, hbm, hbm, vmem, hbm, vmem, vmem],
        out_specs=(vmem, vmem),
        scratch_shapes=[
            pltpu.VMEM((dp_size, rows, depth), bf),
            pltpu.VMEM((dp_size, rows, wide), jnp.float32),
            *halves,
            *halves,
            pltpu.VMEM((rows, depth), bf),
            pltpu.VMEM((units, cache, HD), bf),
            pltpu.VMEM((units, cache, HD), bf),
            dma((units, 2)),
            pltpu.VMEM((depth, wide), bf),
            dma(()),
            pltpu.VMEM((dp_size, rows >> stages, wide), bf),
            pltpu.VMEM((share, mp_size, rows >> stages, wide), bf),
            pltpu.VMEM((dp_size, count, features), bf),
            dma((dp_size, units, 3)),
            dma((dp_size, units)),
            dma((stages, dp_size)),
            dma((stages, dp_size)),
            dma((dp_size,)),
            dma((share, mp_size)),
            dma((dp_size,)),
            dma((dp_size,)),
        ],
        compiler_params=pltpu.CompilerParams(
            collective_id=0, has_side_effects=True, vmem_limit_bytes=VMEM_ALL
        ),
        name="project",
    )(lens, queries, keys, values, cache_k, cache_v, parents, out_weight, residual, picks)


def per_device(
    dp_size,
    mp_size,
    queries,
    tree_keys,
    tree_values,
    cache_keys,
    cache_values,
    cache_lens,
    parents,
    accepted_nodes,
    residual,
    out_weight,
):
    request_count, node_count = parents.shape
    row_base = jnp.arange(request_count, dtype=jnp.int32)[:, None] * node_count
    picks = (row_base + accepted_nodes).reshape(-1, 1)
    return project(
        cache_lens, queries, tree_keys, tree_values, cache_keys, cache_values,
        parents[:, :, None], out_weight, residual, picks, dp_size, mp_size,
    )


def solution(mesh):
    placed = (
        P("dp", "mp"),
        P("dp", "mp"),
        P("dp", "mp"),
        P("dp", None, "mp"),
        P("dp", None, "mp"),
        P("dp"),
        P("dp", None),
        P("dp", None),
        P("dp", "mp"),
        P("mp", "dp"),
    )
    return jax.shard_map(
        functools.partial(per_device, mesh.shape["dp"], mesh.shape["mp"]),
        mesh=mesh,
        in_specs=placed,
        out_specs=(P("dp", "mp"), P(None, "mp")),
        check_vma=False,
    )
```
